1024 devices in a mesh: dp: 16 (over y, core), expert: 64 (over z, x).
Axes of the slice: x: 4, y: 8, z: 16, core: 2. Of those that a mesh axis runs over, the one named last changes fastest.
Arguments:
- tokens: bfloat16 [16, 8192, 4096], P('dp', 'expert'), may hold values from -20 to 20
- router_weight: bfloat16 [4096, 128], replicated
- chosen: int32 [16, 8, 128], P('dp'), may hold values from 0 to 8191, as said below
- w_gate: bfloat16 [4096, 12288], P(None, 'expert'), may hold values from -0.09375 to 0.09375
- w_up: bfloat16 [4096, 12288], P(None, 'expert'), may hold values from -0.09375 to 0.09375
- w_down: bfloat16 [12288, 4096], P('expert'), may hold values from -0.15625 to 0.15625
Outputs:
- combined: bfloat16 [16, 8192, 4096], P('dp', 'expert')
- z_loss: float32 [], replicated
The draws below stay inside these ranges and needn't reach their ends.
Inputs may be any that keep to these rules, and one draw needn't show every extreme that they name: Each list chosen[g, e] holds 128 distinct positions of window g; at most 4 of them lie in any one aligned block of 128 positions (the tokens of one device), and some block holds exactly 4.
All inputs are finite; a program needn't handle non-finite values.
Results may differ from the reference program's by a relative error of at most 0.009.
Values may be sent and summed in bfloat16 or wider, within the bound.
No kernel may reach another device: no remote copies, remote signals or barrier semaphores. Data moves between devices by JAX's collectives and lax.ppermute only.
A program may use at most 64 MiB of HBM per device.

```python
import jax
import jax.numpy as jnp
from jax import lax

D = 4096
FF = 1536
NE = 128
TOK_DEV = 128
CAP = 128
SPLIT = 8
EXPERTS = 8
TOKENS = 8192
MOST = 4
N_DP = 16
N_EXPERT = 64


def chosen_layout(key):
    base = jax.random.fold_in(key, 7001)
    quarter = N_EXPERT // 4
    pattern = jnp.concatenate([jnp.full((quarter,), MOST, jnp.int32), jnp.full((2 * quarter,), MOST // 2, jnp.int32), jnp.zeros((N_EXPERT - 3 * quarter,), jnp.int32)])

    def one_list(group, expert):
        shared = jnp.where(expert == 1, 0, expert)
        group_key = jax.random.fold_in(base, group)
        count_key = jax.random.fold_in(jax.random.fold_in(group_key, 1), shared)
        token_key = jax.random.fold_in(jax.random.fold_in(group_key, 2), shared)
        counts = pattern[jax.random.permutation(count_key, N_EXPERT)]
        counts = jnp.where(expert == 1, jnp.roll(counts, 1), counts)
        orders = jax.vmap(lambda subkey: jax.random.permutation(subkey, TOK_DEV))(jax.random.split(token_key, N_EXPERT))
        orders = orders.astype(jnp.int32)
        owners = jnp.arange(N_EXPERT, dtype=jnp.int32)[:, None] * TOK_DEV
        candidates = (owners + orders[:, :MOST]).reshape(-1)
        live = (jnp.arange(MOST, dtype=jnp.int32)[None, :] < counts[:, None]).reshape(-1)
        ranking = jnp.where(live, 0, 1) * (N_EXPERT * MOST) + jnp.arange(N_EXPERT * MOST, dtype=jnp.int32)
        placing = jnp.argsort(ranking, stable=True)
        return (candidates[placing[:CAP]].astype(jnp.int32), counts, orders[:, 0])
    groups = jnp.arange(N_DP, dtype=jnp.int32)
    experts_all = jnp.arange(EXPERTS, dtype=jnp.int32)
    lists, counts, firsts = jax.vmap(lambda group: jax.vmap(lambda expert: one_list(group, expert))(experts_all))(groups)
    second = 1 if EXPERTS > 1 else 0
    shared_live = ((counts[:, 0] > 0) & (counts[:, second] > 0)).astype(jnp.int32)
    source = jnp.argmax(shared_live, axis=1).astype(jnp.int32)
    aligned = source * TOK_DEV + jnp.take_along_axis(firsts[:, 0], source[:, None], axis=1)[:, 0]
    return (lists, aligned.astype(jnp.int32))


def drawn_vectors(key):
    return jax.random.truncated_normal(jax.random.fold_in(key, 7301), -4.0, 4.0, (N_DP, D), jnp.float32)


def draw_chosen(key, part):
    return chosen_layout(key)[0]


def draw_tokens(key, part):
    lists, aligned = chosen_layout(key)
    value_key = jax.random.fold_in(key, 7101)
    factor_key = jax.random.fold_in(key, 7102)
    position = jnp.arange(N_DP, dtype=jnp.float32)[:, None] * TOKENS + jnp.arange(TOKENS, dtype=jnp.float32)[None, :]
    fraction = position / max(N_DP * TOKENS - 1, 1)
    values = jax.random.truncated_normal(value_key, -4.0, 4.0, (N_DP, TOKENS, D), jnp.float32)
    scale = 0.6 * 5.0 ** fraction
    factor = jnp.exp(jax.random.uniform(factor_key, (N_DP, TOKENS), jnp.float32, -0.35, 0.35))
    values = values * (scale * factor)[:, :, None]
    values = values.at[jnp.arange(N_DP), aligned].set(drawn_vectors(key))
    return values.astype(jnp.bfloat16)


def draw_router_weight(key, part):
    weights = jax.random.truncated_normal(jax.random.fold_in(key, 7201), -4.0, 4.0, (D, NE), jnp.float32) / jnp.sqrt(float(D))
    return weights.astype(jnp.bfloat16)


def block_levels(rng, extent, shards, least, largest):
    level, own = 1.0, jax.random.fold_in(rng, 6)
    for dim, blocks in shards:
        draws = jnp.exp(jax.random.uniform(jax.random.fold_in(own, dim), (blocks,), jnp.float32, least / len(shards), largest / len(shards)))
        level = level * jnp.repeat(draws, extent[dim] // blocks).reshape([-1 if axis == dim else 1 for axis in range(len(extent))])
    return level


def normal_values(rng, shape, deviation, bound, pieces=(), kind=jnp.bfloat16):
    result = deviation * jax.random.normal(rng, shape, jnp.float32)
    if pieces:
        result = result * block_levels(rng, shape, pieces, -0.22, 0.18)
    return jnp.clip(result, -bound, bound).astype(kind)


def setup_inputs(seed: int = 0) -> dict:
    keys = jax.random.split(jax.random.key(seed), 7)
    return {
        "tokens": draw_tokens(jax.random.fold_in(keys[6], 71), 0),
        "router_weight": draw_router_weight(jax.random.fold_in(keys[6], 71), 0),
        "chosen": draw_chosen(jax.random.fold_in(keys[6], 71), 0),
        "w_gate": normal_values(keys[3], (D, EXPERTS * FF), D ** -0.5, 0.09375, ((1, 64),)),
        "w_up": normal_values(keys[4], (D, EXPERTS * FF), D ** -0.5, 0.09375, ((1, 64),)),
        "w_down": normal_values(keys[5], (EXPERTS * FF, D), FF ** -0.5, 0.15625, ((0, 64),)),
    }


def one_window(token_rows, picked, router_weight, w_gate, w_up, w_down):
    logits = jnp.dot(token_rows, router_weight, preferred_element_type=jnp.float32)
    highest = jnp.max(logits, axis=1, keepdims=True)
    log_total = highest[:, 0] + jnp.log(jnp.sum(jnp.exp(logits - highest), axis=1))
    loss_part = jnp.sum(log_total * log_total)
    expert_ids = jnp.arange(EXPERTS, dtype=jnp.int32)
    member = jnp.zeros((TOKENS, EXPERTS), jnp.float32).at[picked, expert_ids[:, None]].set(1.0) > 0.5
    window = logits[:, :EXPERTS]
    peak = jnp.max(jnp.where(member, window, -1e30), axis=1, keepdims=True)
    peak = jnp.where(jnp.any(member, axis=1, keepdims=True), peak, 0.0)
    raised = jnp.where(member, jnp.exp(jnp.where(member, window - peak, -60.0)), 0.0)
    denom = jnp.sum(raised, axis=1, keepdims=True)
    combine = raised / jnp.where(denom > 0, denom, 1.0)
    slice_width = FF // SPLIT

    def expert_step(mixed, expert):
        rows = token_rows[picked[expert]]
        start = (expert * FF).astype(jnp.int32)
        gate_cols = lax.dynamic_slice_in_dim(w_gate, start, FF, 1)
        up_cols = lax.dynamic_slice_in_dim(w_up, start, FF, 1)
        down_rows = lax.dynamic_slice_in_dim(w_down, start, FF, 0)
        gate = jnp.dot(rows, gate_cols, preferred_element_type=jnp.float32)
        upper = jnp.dot(rows, up_cols, preferred_element_type=jnp.float32)
        hidden = (jax.nn.silu(gate) * upper).astype(jnp.bfloat16)
        summed = jnp.zeros((CAP, D), jnp.float32)
        for piece_no in range(SPLIT):
            lower = piece_no * slice_width
            part = jnp.dot(hidden[:, lower:lower + slice_width], down_rows[lower:lower + slice_width], preferred_element_type=jnp.float32)
            part = lax.optimization_barrier(part.astype(jnp.bfloat16))
            summed = summed + part.astype(jnp.float32)
        expert_out = summed.astype(jnp.bfloat16)
        scale = combine[picked[expert], expert]
        mixed = mixed.at[picked[expert]].add(scale[:, None] * expert_out.astype(jnp.float32))
        return mixed, None

    mixed, _ = lax.scan(expert_step, jnp.zeros((TOKENS, D), jnp.float32), expert_ids)
    return mixed.astype(jnp.bfloat16), loss_part


def reference(tokens, router_weight, chosen, w_gate, w_up, w_down):
    def window_fn(pair):
        return one_window(pair[0], pair[1], router_weight, w_gate, w_up, w_down)

    combined, loss_parts = lax.map(window_fn, (tokens, chosen))
    z_loss = jnp.sum(loss_parts) / (N_DP * TOKENS)
    return combined, z_loss
```

```python
import jax
import jax.numpy as jnp
from jax import lax
from jax.sharding import Mesh
from jax.sharding import PartitionSpec as P


DP = ("dp_0", "dp_1")
EXPERT = ("ez", "zp", "x")
SHARE = ("zp", "x")
LANES = 128


def three_terms(value):
    high = value.astype(jnp.bfloat16)
    left = value - high.astype(jnp.float32)
    middle = left.astype(jnp.bfloat16)
    low = (left - middle.astype(jnp.float32)).astype(jnp.bfloat16)
    return jnp.stack([high, middle, low])


def exchange_down(w_down, zp, x, n_zp, n_x, piece):
    rows = w_down.shape[0]
    half = n_x * piece
    other = lax.dynamic_slice(w_down, (0, (1 - zp) * half), (rows, half))
    other = lax.ppermute(other, "zp", [(i, 1 - i) for i in range(n_zp)])
    down = jnp.zeros((n_zp, n_x, rows, piece), w_down.dtype)
    for step in range(n_x):
        block = (x + step) % n_x * piece
        own_part = lax.dynamic_slice(w_down, (0, zp * half + block), (rows, piece))
        part = jnp.stack([own_part, lax.dynamic_slice(other, (0, block), (rows, piece))])
        if step:
            part = lax.ppermute(part, "x", [(i, (i + step) % n_x) for i in range(n_x)])
        source = (x + n_x - step) % n_x
        down = lax.dynamic_update_slice(down, part[0][None, None], (zp, source, 0, 0))
        down = lax.dynamic_update_slice(down, part[1][None, None], (1 - zp, source, 0, 0))
    return down.reshape(n_zp * n_x, rows, piece)


def copy_to(value, axes, count):
    return lax.all_to_all(jnp.broadcast_to(value[None], (count,) + value.shape), axes, 0, 0, tiled=True)


def layer(tokens, router_weight, chosen, w_gate, w_up, w_down):
    token_rows = tokens[0]
    picked = chosen[0]
    experts, cap = picked.shape
    rows_dev, width = token_rows.shape
    devices = lax.axis_size(EXPERT)
    n_dp = lax.axis_size(DP)
    n_zp = lax.axis_size("zp")
    n_x = lax.axis_size("x")
    split = n_zp * n_x
    most = 2 * cap // devices
    piece = width // split
    hidden_cols = w_gate.shape[1]
    me = lax.axis_index(EXPERT)

    local_pos = picked - me * rows_dev
    token_ids = jnp.arange(rows_dev, dtype=jnp.int32)
    member = jnp.any(local_pos[:, :, None] == token_ids[None, None, :], axis=1)
    before = (token_ids[:, None] < token_ids[None, :]).astype(jnp.bfloat16)
    rank = jnp.dot(member.astype(jnp.bfloat16), before, preferred_element_type=jnp.float32)
    slots = jnp.arange(most, dtype=jnp.float32)
    taken = member[:, None, :] & (rank[:, None, :] == slots[None, :, None])
    pick_mat = taken.reshape(experts * most, rows_dev).astype(jnp.bfloat16)
    slot_rows = jnp.dot(pick_mat, token_rows, preferred_element_type=jnp.float32).astype(jnp.bfloat16)
    outgoing = slot_rows.reshape(experts, most, split, piece).transpose(0, 2, 1, 3).reshape(devices, most, piece)
    outgoing, logit_rows, member, taken = lax.optimization_barrier((outgoing, token_rows, member, taken))
    arrived = lax.all_to_all(outgoing, EXPERT, 0, 0, tiled=True)

    down = exchange_down(w_down, lax.axis_index("zp"), lax.axis_index("x"), n_zp, n_x, piece)

    mine = lax.dynamic_index_in_dim(picked, lax.axis_index("ez"), 0, keepdims=False)
    owner = mine // rows_dev
    device_ids = jnp.arange(devices, dtype=jnp.int32)
    first = jnp.sum((owner[None, :] < device_ids[:, None]).astype(jnp.int32), axis=1)
    count = jnp.sum((owner[None, :] == device_ids[:, None]).astype(jnp.int32), axis=1)
    slot_ids = jnp.arange(most, dtype=jnp.int32)[None, :]
    target = jnp.where(slot_ids < count[:, None], first[:, None] + slot_ids, -1).reshape(-1)
    pack_mat = (jnp.arange(cap, dtype=jnp.int32)[:, None] == target[None, :]).astype(jnp.bfloat16)
    packed = jnp.dot(
        pack_mat, arrived.reshape(devices * most, piece), preferred_element_type=jnp.float32
    ).astype(jnp.bfloat16)

    rows = copy_to(packed, SHARE, split)
    gate = jnp.einsum("kpd,kdf->pf", rows, w_gate.reshape(split, piece, hidden_cols), preferred_element_type=jnp.float32)
    upper = jnp.einsum("kpd,kdf->pf", rows, w_up.reshape(split, piece, hidden_cols), preferred_element_type=jnp.float32)
    hidden = (jax.nn.silu(gate) * upper).astype(jnp.bfloat16)
    hidden = copy_to(hidden, SHARE, split)
    expert_out = jnp.einsum("kpf,kfd->pd", hidden, down, preferred_element_type=jnp.float32).astype(jnp.bfloat16)
    spread = lax.dot_general(
        pack_mat, expert_out, (((0,), (0,)), ((), ())), preferred_element_type=jnp.float32
    ).astype(jnp.bfloat16)

    logits = jnp.dot(logit_rows, router_weight, preferred_element_type=jnp.float32)
    highest = jnp.max(logits, axis=1, keepdims=True)
    log_total = highest[:, 0] + jnp.log(jnp.sum(jnp.exp(logits - highest), axis=1))
    loss = jnp.sum(log_total * log_total)
    loss = lax.psum(loss, "dp_1")
    loss = lax.psum(loss, "dp_0")

    terms = jnp.pad(three_terms(loss), (0, LANES - 3))
    terms = jnp.broadcast_to(terms[None, None, :], (devices, most, LANES))
    returned = jnp.concatenate([spread.reshape(devices, most, piece), terms], axis=2)
    returned = lax.all_to_all(returned, EXPERT, 0, 0, tiled=True)
    loss = jnp.sum(returned[:, 0, piece:].astype(jnp.float32))
    z_loss = loss / (n_dp * devices * rows_dev)
    full_out = (
        returned[:, :, :piece].reshape(experts, split, most, piece).transpose(0, 2, 1, 3).reshape(experts * most, width)
    )

    window = logits[:, :experts].T
    peak = jnp.max(jnp.where(member, window, -1e30), axis=0, keepdims=True)
    peak = jnp.where(jnp.any(member, axis=0, keepdims=True), peak, 0.0)
    raised = jnp.where(member, jnp.exp(jnp.where(member, window - peak, -60.0)), 0.0)
    denom = jnp.sum(raised, axis=0, keepdims=True)
    combine = raised / jnp.where(denom > 0, denom, 1.0)
    weights = jnp.where(taken, combine[:, None, :], 0.0).reshape(experts * most, rows_dev)
    coarse = weights.astype(jnp.bfloat16)
    fine = (weights - coarse.astype(jnp.float32)).astype(jnp.bfloat16)
    over_slots = (((0,), (0,)), ((), ()))
    mixed = lax.dot_general(coarse, full_out, over_slots, preferred_element_type=jnp.float32)
    mixed = mixed + lax.dot_general(fine, full_out, over_slots, preferred_element_type=jnp.float32)
    return (mixed.astype(jnp.bfloat16)[None], z_loss)


def solution(mesh):
    split = Mesh(mesh.devices.reshape(8, 2, 8, 2, 4), DP + EXPERT)
    in_specs = (
        P(DP, EXPERT, None),
        P(),
        P(DP, None, None),
        P(None, EXPERT),
        P(None, EXPERT),
        P(EXPERT, None),
    )
    out_specs = (P(DP, EXPERT, None), P())
    return jax.shard_map(layer, mesh=split, in_specs=in_specs, out_specs=out_specs, check_vma=False)
```

```python
import jax
import jax.numpy as jnp
from jax import lax
from jax.sharding import Mesh
from jax.sharding import PartitionSpec as P


DP = ("dp_0", "dp_1")
EXPERT = ("ez", "zp", "x")
SHARE = ("x", "zp")
TRADE = ("ez", "x", "zp")
LANES = 128


def three_terms(value):
    high = value.astype(jnp.bfloat16)
    left = value - high.astype(jnp.float32)
    middle = left.astype(jnp.bfloat16)
    low = (left - middle.astype(jnp.float32)).astype(jnp.bfloat16)
    return jnp.stack([high, middle, low])


def add_partner(value, axis, bit):
    size = lax.axis_size(axis)
    return value + lax.ppermute(value, axis, [(i, i ^ bit) for i in range(size)])


def copy_to(value, axes, count):
    return lax.all_to_all(jnp.broadcast_to(value[None], (count,) + value.shape), axes, 0, 0, tiled=True)


def layer(tokens, router_weight, chosen, w_gate, w_up, w_down):
    token_rows = tokens[0]
    picked = chosen[0]
    experts, cap = picked.shape
    rows_dev, width = token_rows.shape
    devices = lax.axis_size(EXPERT)
    n_dp = lax.axis_size(DP)
    split = lax.axis_size(SHARE)
    most = 2 * cap // devices
    piece = width // split
    hidden_cols = w_gate.shape[1]
    me = lax.axis_index(EXPERT)

    local_pos = picked - me * rows_dev
    token_ids = jnp.arange(rows_dev, dtype=jnp.int32)
    member = jnp.any(local_pos[:, :, None] == token_ids[None, None, :], axis=1)
    before = (token_ids[:, None] < token_ids[None, :]).astype(jnp.bfloat16)
    rank = jnp.dot(member.astype(jnp.bfloat16), before, preferred_element_type=jnp.float32)
    slots = jnp.arange(most, dtype=jnp.float32)
    taken = member[:, None, :] & (rank[:, None, :] == slots[None, :, None])
    pick_mat = taken.reshape(experts * most, rows_dev).astype(jnp.bfloat16)
    slot_rows = jnp.dot(pick_mat, token_rows, preferred_element_type=jnp.float32).astype(jnp.bfloat16)
    outgoing = slot_rows.reshape(experts, most, split, piece).transpose(0, 2, 1, 3).reshape(devices, most, piece)
    outgoing, logit_rows, member, taken = lax.optimization_barrier((outgoing, token_rows, member, taken))
    arrived = lax.all_to_all(outgoing, TRADE, 0, 0, tiled=True)


    mine = lax.dynamic_index_in_dim(picked, lax.axis_index("ez"), 0, keepdims=False)
    owner = mine // rows_dev
    places = jnp.arange(devices, dtype=jnp.int32)
    n_zp = lax.axis_size("zp")
    n_x = lax.axis_size("x")
    device_ids = places // split * split + places % n_zp * n_x + places // n_zp % n_x
    first = jnp.sum((owner[None, :] < device_ids[:, None]).astype(jnp.int32), axis=1)
    count = jnp.sum((owner[None, :] == device_ids[:, None]).astype(jnp.int32), axis=1)
    slot_ids = jnp.arange(most, dtype=jnp.int32)[None, :]
    target = jnp.where(slot_ids < count[:, None], first[:, None] + slot_ids, -1).reshape(-1)
    pack_mat = (jnp.arange(cap, dtype=jnp.int32)[:, None] == target[None, :]).astype(jnp.bfloat16)
    packed = jnp.dot(
        pack_mat, arrived.reshape(devices * most, piece), preferred_element_type=jnp.float32
    ).astype(jnp.bfloat16)

    rows = copy_to(packed, SHARE, split)
    gate = jnp.einsum("kpd,kdf->pf", rows, w_gate.reshape(split, piece, hidden_cols), preferred_element_type=jnp.float32)
    upper = jnp.einsum("kpd,kdf->pf", rows, w_up.reshape(split, piece, hidden_cols), preferred_element_type=jnp.float32)
    hidden = (jax.nn.silu(gate) * upper).astype(jnp.bfloat16)
    parts = jnp.einsum(
        "pf,fkd->kpd", hidden, w_down.reshape(hidden_cols, split, piece), preferred_element_type=jnp.float32
    ).astype(jnp.bfloat16)
    parts = lax.all_to_all(parts, SHARE, 0, 0, tiled=True)
    expert_out = jnp.sum(parts.astype(jnp.float32), axis=0).astype(jnp.bfloat16)
    spread = lax.dot_general(
        pack_mat, expert_out, (((0,), (0,)), ((), ())), preferred_element_type=jnp.float32
    ).astype(jnp.bfloat16)

    logits = jnp.dot(logit_rows, router_weight, preferred_element_type=jnp.float32)
    highest = jnp.max(logits, axis=1, keepdims=True)
    log_total = highest[:, 0] + jnp.log(jnp.sum(jnp.exp(logits - highest), axis=1))
    loss = jnp.sum(log_total * log_total)
    loss = lax.psum(loss, "dp_1")
    loss = jnp.broadcast_to(loss, (8, LANES))
    loss = add_partner(loss, "dp_0", 1)
    loss = add_partner(loss, "dp_0", 2)
    loss = add_partner(loss, "dp_0", 4)
    loss = loss[0, 0]

    terms = jnp.pad(three_terms(loss), (0, LANES - 3))
    terms = jnp.broadcast_to(terms[None, None, :], (devices, most, LANES))
    returned = jnp.concatenate([spread.reshape(devices, most, piece), terms], axis=2)
    returned = lax.all_to_all(returned, TRADE, 0, 0, tiled=True)
    loss = jnp.sum(returned[:, 0, piece:].astype(jnp.float32))
    z_loss = loss / (n_dp * devices * rows_dev)
    full_out = (
        returned[:, :, :piece].reshape(experts, split, most, piece).transpose(0, 2, 1, 3).reshape(experts * most, width)
    )

    window = logits[:, :experts].T
    peak = jnp.max(jnp.where(member, window, -1e30), axis=0, keepdims=True)
    peak = jnp.where(jnp.any(member, axis=0, keepdims=True), peak, 0.0)
    raised = jnp.where(member, jnp.exp(jnp.where(member, window - peak, -60.0)), 0.0)
    denom = jnp.sum(raised, axis=0, keepdims=True)
    combine = raised / jnp.where(denom > 0, denom, 1.0)
    weights = jnp.where(taken, combine[:, None, :], 0.0).reshape(experts * most, rows_dev)
    coarse = weights.astype(jnp.bfloat16)
    fine = (weights - coarse.astype(jnp.float32)).astype(jnp.bfloat16)
    mixed = lax.dot_general(
        jnp.concatenate([coarse, fine]),
        jnp.concatenate([full_out, full_out]),
        (((0,), (0,)), ((), ())),
        preferred_element_type=jnp.float32,
    )
    return (mixed.astype(jnp.bfloat16)[None], z_loss)


def solution(mesh):
    split = Mesh(mesh.devices.reshape(8, 2, 8, 2, 4), DP + EXPERT)
    in_specs = (
        P(DP, EXPERT, None),
        P(),
        P(DP, None, None),
        P(None, EXPERT),
        P(None, EXPERT),
        P(EXPERT, None),
    )
    out_specs = (P(DP, EXPERT, None), P())
    return jax.shard_map(layer, mesh=split, in_specs=in_specs, out_specs=out_specs, check_vma=False)
```

```python
import jax
import jax.numpy as jnp
from jax import lax
from jax.sharding import Mesh
from jax.sharding import PartitionSpec as P


DP = ("dp_0", "dp_1")
EXPERT = ("ez", "zp", "x")
SHARE = ("x", "zp")
TRADE = ("ez", "x", "zp")
LANES = 128


def three_terms(value):
    high = value.astype(jnp.bfloat16)
    left = value - high.astype(jnp.float32)
    middle = left.astype(jnp.bfloat16)
    low = (left - middle.astype(jnp.float32)).astype(jnp.bfloat16)
    return jnp.stack([high, middle, low])


def add_partner(value, axis, bit):
    size = lax.axis_size(axis)
    return value + lax.ppermute(value, axis, [(i, i ^ bit) for i in range(size)])


def exchange_down(w_down, later, core, zp, x, n_core, n_zp, n_x):
    rows, width = w_down.shape
    piece = width // (n_x * n_zp)
    half = piece // n_core

    def columns(weight, column, row):
        return lax.dynamic_slice(weight, (0, (column * n_zp + row) * piece + core * half), (rows, half))

    other = jnp.concatenate([columns(w_down, column, 1 - zp) for column in range(n_x)], axis=1)
    other = lax.ppermute(other, "zp", [(i, 1 - i) for i in range(n_zp)])
    mine = jnp.zeros((n_x * n_zp, rows, half), w_down.dtype)
    for step in range(n_x):
        target = (x + step) % n_x
        own_part = columns(later, target, zp)
        other_part = lax.dynamic_slice(other, (0, target * half), (rows, half))
        part = jnp.stack([jnp.where(zp == 0, own_part, other_part), jnp.where(zp == 0, other_part, own_part)])
        if step:
            part = lax.ppermute(part, "x", [(i, (i + step) % n_x) for i in range(n_x)])
        mine = lax.dynamic_update_slice(mine, part, ((x + n_x - step) % n_x * n_zp, 0, 0))
    theirs = lax.ppermute(mine, "dp_1", [(i, 1 - i) for i in range(n_core)])
    return mine, theirs


def copy_to(value, axes, count):
    return lax.all_to_all(jnp.broadcast_to(value[None], (count,) + value.shape), axes, 0, 0, tiled=True)


def layer(tokens, router_weight, chosen, w_gate, w_up, w_down):
    token_rows = tokens[0]
    picked = chosen[0]
    experts, cap = picked.shape
    rows_dev, width = token_rows.shape
    devices = lax.axis_size(EXPERT)
    n_dp = lax.axis_size(DP)
    split = lax.axis_size(SHARE)
    most = 2 * cap // devices
    piece = width // split
    hidden_cols = w_gate.shape[1]
    me = lax.axis_index(EXPERT)

    local_pos = picked - me * rows_dev
    token_ids = jnp.arange(rows_dev, dtype=jnp.int32)
    member = jnp.any(local_pos[:, :, None] == token_ids[None, None, :], axis=1)
    before = (token_ids[:, None] < token_ids[None, :]).astype(jnp.bfloat16)
    rank = jnp.dot(member.astype(jnp.bfloat16), before, preferred_element_type=jnp.float32)
    slots = jnp.arange(most, dtype=jnp.float32)
    taken = member[:, None, :] & (rank[:, None, :] == slots[None, :, None])
    pick_mat = taken.reshape(experts * most, rows_dev).astype(jnp.bfloat16)
    slot_rows = jnp.dot(pick_mat, token_rows, preferred_element_type=jnp.float32).astype(jnp.bfloat16)
    logits = jnp.dot(token_rows, router_weight, preferred_element_type=jnp.float32)
    highest = jnp.max(logits, axis=1, keepdims=True)
    log_total = highest[:, 0] + jnp.log(jnp.sum(jnp.exp(logits - highest), axis=1))

    terms = jnp.pad(three_terms(log_total * log_total), ((0, most - 3), (0, 0)))
    outgoing = slot_rows.reshape(experts, most, split, piece).transpose(0, 2, 1, 3).reshape(devices, most, piece)
    outgoing = jnp.concatenate([outgoing, jnp.broadcast_to(terms[None], (devices, most, rows_dev))], axis=2)
    outgoing, logits, member, taken, later = lax.optimization_barrier((outgoing, logits, member, taken, w_down))
    arrived = lax.all_to_all(outgoing, TRADE, 0, 0, tiled=True)
    core, zp, x = (lax.axis_index(name) for name in ("dp_1", "zp", "x"))
    n_core, n_zp, n_x = (lax.axis_size(name) for name in ("dp_1", "zp", "x"))
    down_mine, down_theirs = exchange_down(w_down, later, core, zp, x, n_core, n_zp, n_x)

    mine = lax.dynamic_index_in_dim(picked, lax.axis_index("ez"), 0, keepdims=False)
    owner = mine // rows_dev
    places = jnp.arange(devices, dtype=jnp.int32)
    device_ids = places // split * split + places % n_zp * n_x + places // n_zp % n_x
    first = jnp.sum((owner[None, :] < device_ids[:, None]).astype(jnp.int32), axis=1)
    count = jnp.sum((owner[None, :] == device_ids[:, None]).astype(jnp.int32), axis=1)
    slot_ids = jnp.arange(most, dtype=jnp.int32)[None, :]
    target = jnp.where(slot_ids < count[:, None], first[:, None] + slot_ids, -1).reshape(-1)
    pack_mat = (jnp.arange(cap, dtype=jnp.int32)[:, None] == target[None, :]).astype(jnp.bfloat16)
    packed = jnp.dot(
        pack_mat, arrived[:, :, :piece].reshape(devices * most, piece), preferred_element_type=jnp.float32
    ).astype(jnp.bfloat16)

    rows = copy_to(packed, SHARE, split)
    gate = jnp.einsum("kpd,kdf->pf", rows, w_gate.reshape(split, piece, hidden_cols), preferred_element_type=jnp.float32)
    upper = jnp.einsum("kpd,kdf->pf", rows, w_up.reshape(split, piece, hidden_cols), preferred_element_type=jnp.float32)
    hidden = (jax.nn.silu(gate) * upper).astype(jnp.bfloat16)
    hidden = copy_to(hidden, SHARE, split)
    out_mine = jnp.einsum("kpf,kfd->pd", hidden, down_mine, preferred_element_type=jnp.float32).astype(jnp.bfloat16)
    out_theirs = jnp.einsum("kpf,kfd->pd", hidden, down_theirs, preferred_element_type=jnp.float32).astype(jnp.bfloat16)
    low = jnp.where(core == 0, out_mine, out_theirs)
    high = jnp.where(core == 0, out_theirs, out_mine)
    expert_out = jnp.concatenate([low, high], axis=1)
    spread = lax.dot_general(
        pack_mat, expert_out, (((0,), (0,)), ((), ())), preferred_element_type=jnp.float32
    ).astype(jnp.bfloat16)

    returned = lax.all_to_all(spread.reshape(devices, most, piece), TRADE, 0, 0, tiled=True)
    full_out = returned.reshape(experts, split, most, piece).transpose(0, 2, 1, 3).reshape(experts * most, width)

    loss = jnp.sum(arrived[:, :, piece:].astype(jnp.float32))
    loss = lax.psum(loss, "dp_1")
    loss = jnp.broadcast_to(loss, (8, LANES))
    loss = add_partner(loss, "dp_0", 1)
    loss = add_partner(loss, "dp_0", 2)
    loss = add_partner(loss, "dp_0", 4)
    z_loss = loss[0, 0] / (n_dp * devices * rows_dev)

    window = logits[:, :experts].T
    peak = jnp.max(jnp.where(member, window, -1e30), axis=0, keepdims=True)
    peak = jnp.where(jnp.any(member, axis=0, keepdims=True), peak, 0.0)
    raised = jnp.where(member, jnp.exp(jnp.where(member, window - peak, -60.0)), 0.0)
    denom = jnp.sum(raised, axis=0, keepdims=True)
    combine = raised / jnp.where(denom > 0, denom, 1.0)
    weights = jnp.where(taken, combine[:, None, :], 0.0).reshape(experts * most, rows_dev)
    coarse = weights.astype(jnp.bfloat16)
    fine = (weights - coarse.astype(jnp.float32)).astype(jnp.bfloat16)
    mixed = lax.dot_general(
        jnp.concatenate([coarse, fine]),
        jnp.concatenate([full_out, full_out]),
        (((0,), (0,)), ((), ())),
        preferred_element_type=jnp.float32,
    )
    return (mixed.astype(jnp.bfloat16)[None], z_loss)


def solution(mesh):
    split = Mesh(mesh.devices.reshape(8, 2, 8, 2, 4), DP + EXPERT)
    in_specs = (
        P(DP, EXPERT, None),
        P(),
        P(DP, None, None),
        P(None, EXPERT),
        P(None, EXPERT),
        P(EXPERT, None),
    )
    out_specs = (P(DP, EXPERT, None), P())
    return jax.shard_map(layer, mesh=split, in_specs=in_specs, out_specs=out_specs, check_vma=False)
```

```python
import jax
import jax.numpy as jnp
from jax import lax
from jax.sharding import Mesh
from jax.sharding import PartitionSpec as P


DP = ("dp_0", "dp_1")
EXPERT = ("ez", "zp", "x")
SHARE = ("x", "zp")
TRADE = ("ez", "x", "zp")
LANES = 128


def three_terms(value):
    high = value.astype(jnp.bfloat16)
    left = value - high.astype(jnp.float32)
    middle = left.astype(jnp.bfloat16)
    low = (left - middle.astype(jnp.float32)).astype(jnp.bfloat16)
    return jnp.stack([high, middle, low])


def add_partner(value, axis, bit):
    size = lax.axis_size(axis)
    return value + lax.ppermute(value, axis, [(i, i ^ bit) for i in range(size)])


def exchange_down(w_down, later, core, zp, x, n_core, n_zp, n_x):
    rows, width = w_down.shape
    piece = width // (n_x * n_zp)
    half = piece // n_core

    def columns(weight, column, row):
        return lax.dynamic_slice(weight, (0, (column * n_zp + row) * piece + core * half), (rows, half))

    other = jnp.concatenate([columns(w_down, column, 1 - zp) for column in range(n_x)], axis=1)
    other = lax.ppermute(other, "zp", [(i, 1 - i) for i in range(n_zp)])
    mine = jnp.zeros((n_x * n_zp, rows, half), w_down.dtype)
    for step in range(n_x):
        target = (x + step) % n_x
        own_part = columns(later, target, zp)
        other_part = lax.dynamic_slice(other, (0, target * half), (rows, half))
        part = jnp.stack([jnp.where(zp == 0, own_part, other_part), jnp.where(zp == 0, other_part, own_part)])
        if step:
            part = lax.ppermute(part, "x", [(i, (i + step) % n_x) for i in range(n_x)])
        mine = lax.dynamic_update_slice(mine, part, ((x + n_x - step) % n_x * n_zp, 0, 0))
    theirs = lax.ppermute(mine, "dp_1", [(i, 1 - i) for i in range(n_core)])
    return mine, theirs


def copy_to(value, axes, count):
    return lax.all_to_all(jnp.broadcast_to(value[None], (count,) + value.shape), axes, 0, 0, tiled=True)


def layer(tokens, router_weight, chosen, w_gate, w_up, w_down):
    token_rows = tokens[0]
    picked = chosen[0]
    experts, cap = picked.shape
    rows_dev, width = token_rows.shape
    devices = lax.axis_size(EXPERT)
    n_dp = lax.axis_size(DP)
    split = lax.axis_size(SHARE)
    most = 2 * cap // devices
    piece = width // split
    hidden_cols = w_gate.shape[1]
    me = lax.axis_index(EXPERT)

    local_pos = picked - me * rows_dev
    token_ids = jnp.arange(rows_dev, dtype=jnp.int32)
    member = jnp.any(local_pos[:, :, None] == token_ids[None, None, :], axis=1)
    before = (token_ids[:, None] < token_ids[None, :]).astype(jnp.bfloat16)
    rank = jnp.dot(member.astype(jnp.bfloat16), before, preferred_element_type=jnp.float32)
    slots = jnp.arange(most, dtype=jnp.float32)
    taken = member[:, None, :] & (rank[:, None, :] == slots[None, :, None])
    pick_mat = taken.reshape(experts * most, rows_dev).astype(jnp.bfloat16)
    slot_rows = jnp.dot(pick_mat, token_rows, preferred_element_type=jnp.float32).astype(jnp.bfloat16)
    logits = jnp.dot(token_rows, router_weight, preferred_element_type=jnp.float32)
    highest = jnp.max(logits, axis=1, keepdims=True)
    log_total = highest[:, 0] + jnp.log(jnp.sum(jnp.exp(logits - highest), axis=1))

    terms = jnp.pad(three_terms(log_total * log_total), ((0, most - 3), (0, 0)))
    outgoing = slot_rows.reshape(experts, most, split, piece).transpose(0, 2, 1, 3).reshape(devices, most, piece)
    outgoing = jnp.concatenate([outgoing, jnp.broadcast_to(terms[None], (devices, most, rows_dev))], axis=2)
    outgoing, logits, member, taken, later = lax.optimization_barrier((outgoing, logits, member, taken, w_down))
    arrived = lax.all_to_all(outgoing, TRADE, 0, 0, tiled=True)
    core, zp, x = (lax.axis_index(name) for name in ("dp_1", "zp", "x"))
    n_core, n_zp, n_x = (lax.axis_size(name) for name in ("dp_1", "zp", "x"))
    down_mine, down_theirs = exchange_down(w_down, later, core, zp, x, n_core, n_zp, n_x)

    mine = lax.dynamic_index_in_dim(picked, lax.axis_index("ez"), 0, keepdims=False)
    owner = mine // rows_dev
    places = jnp.arange(devices, dtype=jnp.int32)
    device_ids = places // split * split + places % n_zp * n_x + places // n_zp % n_x
    first = jnp.sum((owner[None, :] < device_ids[:, None]).astype(jnp.int32), axis=1)
    count = jnp.sum((owner[None, :] == device_ids[:, None]).astype(jnp.int32), axis=1)
    slot_ids = jnp.arange(most, dtype=jnp.int32)[None, :]
    target = jnp.where(slot_ids < count[:, None], first[:, None] + slot_ids, -1).reshape(-1)
    pack_mat = (jnp.arange(cap, dtype=jnp.int32)[:, None] == target[None, :]).astype(jnp.bfloat16)
    copy_mat = (jnp.arange(split * cap, dtype=jnp.int32)[:, None] % cap == target[None, :]).astype(jnp.bfloat16)
    packed = jnp.dot(
        copy_mat, arrived[:, :, :piece].reshape(devices * most, piece), preferred_element_type=jnp.float32
    ).astype(jnp.bfloat16)

    rows = lax.all_to_all(packed.reshape(split, cap, piece), SHARE, 0, 0, tiled=True)
    gate = jnp.einsum("kpd,kdf->pf", rows, w_gate.reshape(split, piece, hidden_cols), preferred_element_type=jnp.float32)
    upper = jnp.einsum("kpd,kdf->pf", rows, w_up.reshape(split, piece, hidden_cols), preferred_element_type=jnp.float32)
    hidden = (jax.nn.silu(gate) * upper).astype(jnp.bfloat16)
    hidden = copy_to(hidden, SHARE, split)
    out_mine = jnp.einsum("kpf,kfd->pd", hidden, down_mine, preferred_element_type=jnp.float32).astype(jnp.bfloat16)
    out_theirs = jnp.einsum("kpf,kfd->pd", hidden, down_theirs, preferred_element_type=jnp.float32).astype(jnp.bfloat16)
    low = jnp.where(core == 0, out_mine, out_theirs)
    high = jnp.where(core == 0, out_theirs, out_mine)
    expert_out = jnp.concatenate([low, high], axis=1)
    spread = lax.dot_general(
        pack_mat, expert_out, (((0,), (0,)), ((), ())), preferred_element_type=jnp.float32
    ).astype(jnp.bfloat16)

    returned = lax.all_to_all(spread.reshape(devices, most, piece), TRADE, 0, 0, tiled=True)
    full_out = returned.reshape(experts, split, most, piece).transpose(0, 2, 1, 3).reshape(experts * most, width)

    loss = jnp.sum(arrived[:, :, piece:].astype(jnp.float32))
    loss = jnp.broadcast_to(loss, (8, LANES))
    loss = add_partner(loss, "dp_0", 1)
    loss = lax.psum(loss, "dp_1")
    loss = add_partner(loss, "dp_0", 2)
    loss = add_partner(loss, "dp_0", 4)
    z_loss = loss[0, 0] / (n_dp * devices * rows_dev)

    window = logits[:, :experts].T
    peak = jnp.max(jnp.where(member, window, -1e30), axis=0, keepdims=True)
    peak = jnp.where(jnp.any(member, axis=0, keepdims=True), peak, 0.0)
    raised = jnp.where(member, jnp.exp(jnp.where(member, window - peak, -60.0)), 0.0)
    denom = jnp.sum(raised, axis=0, keepdims=True)
    combine = raised / jnp.where(denom > 0, denom, 1.0)
    weights = jnp.where(taken, combine[:, None, :], 0.0).reshape(experts * most, rows_dev)
    coarse = weights.astype(jnp.bfloat16)
    fine = (weights - coarse.astype(jnp.float32)).astype(jnp.bfloat16)
    mixed = lax.dot_general(
        jnp.concatenate([coarse, fine]),
        jnp.concatenate([full_out, full_out]),
        (((0,), (0,)), ((), ())),
        preferred_element_type=jnp.float32,
    )
    return (mixed.astype(jnp.bfloat16)[None], z_loss)


def solution(mesh):
    split = Mesh(mesh.devices.reshape(8, 2, 8, 2, 4), DP + EXPERT)
    in_specs = (
        P(DP, EXPERT, None),
        P(),
        P(DP, None, None),
        P(None, EXPERT),
        P(None, EXPERT),
        P(EXPERT, None),
    )
    out_specs = (P(DP, EXPERT, None), P())
    return jax.shard_map(layer, mesh=split, in_specs=in_specs, out_specs=out_specs, check_vma=False)
```

```python
import jax
import jax.numpy as jnp
from jax import lax
from jax.sharding import Mesh
from jax.sharding import PartitionSpec as P


DP = ("dp_0", "dp_1")
EXPERT = ("ez", "zp", "x")
SHARE = ("x", "zp")
TRADE = ("ez", "x", "zp")
LANES = 128


def three_terms(value):
    high = value.astype(jnp.bfloat16)
    left = value - high.astype(jnp.float32)
    middle = left.astype(jnp.bfloat16)
    low = (left - middle.astype(jnp.float32)).astype(jnp.bfloat16)
    return jnp.stack([high, middle, low])


def add_partner(value, axis, bit):
    size = lax.axis_size(axis)
    return value + lax.ppermute(value, axis, [(i, i ^ bit) for i in range(size)])


def exchange_down(w_down, later, core, zp, x, n_core, n_zp, n_x):
    rows, width = w_down.shape
    piece = width // (n_x * n_zp)
    half = piece // n_core

    def columns(weight, column, row):
        return lax.dynamic_slice(weight, (0, (column * n_zp + row) * piece + core * half), (rows, half))

    other = jnp.concatenate([columns(w_down, column, 1 - zp) for column in range(n_x)], axis=1)
    other = lax.ppermute(other, "zp", [(i, 1 - i) for i in range(n_zp)])
    mine = jnp.zeros((n_x * n_zp, rows, half), w_down.dtype)
    for step in range(n_x):
        target = (x + step) % n_x
        own_part = columns(later, target, zp)
        other_part = lax.dynamic_slice(other, (0, target * half), (rows, half))
        part = jnp.stack([jnp.where(zp == 0, own_part, other_part), jnp.where(zp == 0, other_part, own_part)])
        if step:
            part = lax.ppermute(part, "x", [(i, (i + step) % n_x) for i in range(n_x)])
        mine = lax.dynamic_update_slice(mine, part, ((x + n_x - step) % n_x * n_zp, 0, 0))
    theirs = lax.ppermute(mine, "dp_1", [(i, 1 - i) for i in range(n_core)])
    return mine, theirs


def copy_to(value, axes, count):
    return lax.all_to_all(jnp.broadcast_to(value[None], (count,) + value.shape), axes, 0, 0, tiled=True)


def layer(tokens, router_weight, chosen, w_gate, w_up, w_down):
    token_rows = tokens[0]
    picked = chosen[0]
    experts, cap = picked.shape
    rows_dev, width = token_rows.shape
    devices = lax.axis_size(EXPERT)
    n_dp = lax.axis_size(DP)
    split = lax.axis_size(SHARE)
    most = 2 * cap // devices
    piece = width // split
    hidden_cols = w_gate.shape[1]
    me = lax.axis_index(EXPERT)

    local_pos = picked - me * rows_dev
    token_ids = jnp.arange(rows_dev, dtype=jnp.int32)
    member = jnp.any(local_pos[:, :, None] == token_ids[None, None, :], axis=1)
    before = (token_ids[:, None] < token_ids[None, :]).astype(jnp.bfloat16)
    rank = jnp.dot(member.astype(jnp.bfloat16), before, preferred_element_type=jnp.float32)
    slots = jnp.arange(most, dtype=jnp.float32)
    taken = member[:, None, :] & (rank[:, None, :] == slots[None, :, None])
    pick_mat = taken.reshape(experts * most, rows_dev).astype(jnp.bfloat16)
    slot_rows = jnp.dot(pick_mat, token_rows, preferred_element_type=jnp.float32).astype(jnp.bfloat16)
    logits = jnp.dot(token_rows, router_weight, preferred_element_type=jnp.float32)
    highest = jnp.max(logits, axis=1, keepdims=True)
    log_total = highest[:, 0] + jnp.log(jnp.sum(jnp.exp(logits - highest), axis=1))

    terms = jnp.pad(three_terms(log_total * log_total), ((0, most - 3), (0, 0)))
    outgoing = slot_rows.reshape(experts, most, split, piece).transpose(0, 2, 1, 3).reshape(devices, most, piece)
    outgoing = jnp.concatenate([outgoing, jnp.broadcast_to(terms[None], (devices, most, rows_dev))], axis=2)
    outgoing, logits, member, taken, later = lax.optimization_barrier((outgoing, logits, member, taken, w_down))
    arrived = lax.all_to_all(outgoing, TRADE, 0, 0, tiled=True)
    core, zp, x = (lax.axis_index(name) for name in ("dp_1", "zp", "x"))
    n_core, n_zp, n_x = (lax.axis_size(name) for name in ("dp_1", "zp", "x"))
    down_mine, down_theirs = exchange_down(w_down, later, core, zp, x, n_core, n_zp, n_x)

    mine = lax.dynamic_index_in_dim(picked, lax.axis_index("ez"), 0, keepdims=False)
    owner = mine // rows_dev
    places = jnp.arange(devices, dtype=jnp.int32)
    device_ids = places // split * split + places % n_zp * n_x + places // n_zp % n_x
    first = jnp.sum((owner[None, :] < device_ids[:, None]).astype(jnp.int32), axis=1)
    count = jnp.sum((owner[None, :] == device_ids[:, None]).astype(jnp.int32), axis=1)
    slot_ids = jnp.arange(most, dtype=jnp.int32)[None, :]
    target = jnp.where(slot_ids < count[:, None], first[:, None] + slot_ids, -1).reshape(-1)
    pack_mat = (jnp.arange(cap, dtype=jnp.int32)[:, None] == target[None, :]).astype(jnp.bfloat16)
    packed = jnp.dot(
        pack_mat, arrived[:, :, :piece].reshape(devices * most, piece), preferred_element_type=jnp.float32
    ).astype(jnp.bfloat16)

    rows = copy_to(packed, SHARE, split)
    gate = jnp.einsum("kpd,kdf->pf", rows, w_gate.reshape(split, piece, hidden_cols), preferred_element_type=jnp.float32)
    upper = jnp.einsum("kpd,kdf->pf", rows, w_up.reshape(split, piece, hidden_cols), preferred_element_type=jnp.float32)
    hidden = (jax.nn.silu(gate) * upper).astype(jnp.bfloat16)
    hidden, down_theirs, first_core = lax.optimization_barrier((hidden, down_theirs, core == 0))
    hidden = copy_to(hidden, SHARE, split)
    out_mine = jnp.einsum("kpf,kfd->pd", hidden, down_mine, preferred_element_type=jnp.float32).astype(jnp.bfloat16)
    out_theirs = jnp.einsum("kpf,kfd->pd", hidden, down_theirs, preferred_element_type=jnp.float32).astype(jnp.bfloat16)
    low = jnp.where(first_core, out_mine, out_theirs)
    high = jnp.where(first_core, out_theirs, out_mine)
    expert_out = jnp.concatenate([low, high], axis=1)
    spread = lax.dot_general(
        pack_mat, expert_out, (((0,), (0,)), ((), ())), preferred_element_type=jnp.float32
    ).astype(jnp.bfloat16)

    returned = lax.all_to_all(spread.reshape(devices, most, piece), TRADE, 0, 0, tiled=True)
    full_out = returned.reshape(experts, split, most, piece).transpose(0, 2, 1, 3).reshape(experts * most, width)

    loss = jnp.sum(arrived[:, :, piece:].astype(jnp.float32))
    loss = jnp.broadcast_to(loss, (8, LANES))
    loss = add_partner(loss, "dp_0", 1)
    loss = lax.psum(loss, "dp_1")
    loss = add_partner(loss, "dp_0", 2)
    loss = add_partner(loss, "dp_0", 4)
    z_loss = loss[0, 0] / (n_dp * devices * rows_dev)

    window = logits[:, :experts].T
    peak = jnp.max(jnp.where(member, window, -1e30), axis=0, keepdims=True)
    peak = jnp.where(jnp.any(member, axis=0, keepdims=True), peak, 0.0)
    raised = jnp.where(member, jnp.exp(jnp.where(member, window - peak, -60.0)), 0.0)
    denom = jnp.sum(raised, axis=0, keepdims=True)
    combine = raised / jnp.where(denom > 0, denom, 1.0)
    weights = jnp.where(taken, combine[:, None, :], 0.0).reshape(experts * most, rows_dev)
    coarse = weights.astype(jnp.bfloat16)
    fine = (weights - coarse.astype(jnp.float32)).astype(jnp.bfloat16)
    mixed = lax.dot_general(
        jnp.concatenate([coarse, fine]),
        jnp.concatenate([full_out, full_out]),
        (((0,), (0,)), ((), ())),
        preferred_element_type=jnp.float32,
    )
    return (mixed.astype(jnp.bfloat16)[None], z_loss)


def solution(mesh):
    split = Mesh(mesh.devices.reshape(8, 2, 8, 2, 4), DP + EXPERT)
    in_specs = (
        P(DP, EXPERT, None),
        P(),
        P(DP, None, None),
        P(None, EXPERT),
        P(None, EXPERT),
        P(EXPERT, None),
    )
    out_specs = (P(DP, EXPERT, None), P())
    return jax.shard_map(layer, mesh=split, in_specs=in_specs, out_specs=out_specs, check_vma=False)
```

```python
import jax
import jax.numpy as jnp
from jax import lax
from jax.sharding import Mesh
from jax.sharding import PartitionSpec as P


DP = ("dp_0", "dp_1")
EXPERT = ("ez", "zp", "x")
SHARE = ("x", "zp")
TRADE = ("ez", "x", "zp")


def three_terms(value):
    high = value.astype(jnp.bfloat16)
    left = value - high.astype(jnp.float32)
    middle = left.astype(jnp.bfloat16)
    low = (left - middle.astype(jnp.float32)).astype(jnp.bfloat16)
    return jnp.stack([high, middle, low])


def add_partner(value, axis, bit):
    size = lax.axis_size(axis)
    return value + lax.ppermute(value, axis, [(i, i ^ bit) for i in range(size)])


def exchange_down(w_down, later, core, zp, x, n_core, n_zp, n_x):
    rows, width = w_down.shape
    piece = width // (n_x * n_zp)
    half = piece // n_core

    def columns(weight, column, row):
        return lax.dynamic_slice(weight, (0, (column * n_zp + row) * piece + core * half), (rows, half))

    other = jnp.concatenate([columns(w_down, column, 1 - zp) for column in range(n_x)], axis=1)
    other = lax.ppermute(other, "zp", [(i, 1 - i) for i in range(n_zp)])
    mine = jnp.zeros((n_x * n_zp, rows, half), w_down.dtype)
    for step in range(n_x):
        target = (x + step) % n_x
        own_part = columns(later, target, zp)
        other_part = lax.dynamic_slice(other, (0, target * half), (rows, half))
        part = jnp.stack([jnp.where(zp == 0, own_part, other_part), jnp.where(zp == 0, other_part, own_part)])
        if step:
            part = lax.ppermute(part, "x", [(i, (i + step) % n_x) for i in range(n_x)])
        mine = lax.dynamic_update_slice(mine, part, ((x + n_x - step) % n_x * n_zp, 0, 0))
    theirs = lax.ppermute(mine, "dp_1", [(i, 1 - i) for i in range(n_core)])
    return mine, theirs


def copy_to(value, axes, count):
    return lax.all_to_all(jnp.broadcast_to(value[None], (count,) + value.shape), axes, 0, 0, tiled=True)


def layer(tokens, router_weight, chosen, w_gate, w_up, w_down):
    token_rows = tokens[0]
    picked = chosen[0]
    experts, cap = picked.shape
    rows_dev, width = token_rows.shape
    devices = lax.axis_size(EXPERT)
    n_dp = lax.axis_size(DP)
    split = lax.axis_size(SHARE)
    most = 2 * cap // devices
    piece = width // split
    hidden_cols = w_gate.shape[1]
    me = lax.axis_index(EXPERT)

    local_pos = picked - me * rows_dev
    token_ids = jnp.arange(rows_dev, dtype=jnp.int32)
    member = jnp.any(local_pos[:, :, None] == token_ids[None, None, :], axis=1)
    before = (token_ids[:, None] < token_ids[None, :]).astype(jnp.bfloat16)
    rank = jnp.dot(member.astype(jnp.bfloat16), before, preferred_element_type=jnp.float32)
    slots = jnp.arange(most, dtype=jnp.float32)
    taken = member[:, None, :] & (rank[:, None, :] == slots[None, :, None])
    pick_mat = taken.reshape(experts * most, rows_dev).astype(jnp.bfloat16)
    slot_rows = jnp.dot(pick_mat, token_rows, preferred_element_type=jnp.float32).astype(jnp.bfloat16)
    logits = jnp.dot(token_rows, router_weight, preferred_element_type=jnp.float32)
    highest = jnp.max(logits, axis=1, keepdims=True)
    log_total = highest[:, 0] + jnp.log(jnp.sum(jnp.exp(logits - highest), axis=1))

    terms = jnp.pad(three_terms(log_total * log_total), ((0, most - 3), (0, 0)))
    outgoing = slot_rows.reshape(experts, most, split, piece).transpose(0, 2, 1, 3).reshape(devices, most, piece)
    outgoing = jnp.concatenate([outgoing, jnp.broadcast_to(terms[None], (devices, most, rows_dev))], axis=2)
    outgoing, logits, member, taken, later = lax.optimization_barrier((outgoing, logits, member, taken, w_down))
    arrived = lax.all_to_all(outgoing, TRADE, 0, 0, tiled=True)
    core, zp, x = (lax.axis_index(name) for name in ("dp_1", "zp", "x"))
    n_core, n_zp, n_x = (lax.axis_size(name) for name in ("dp_1", "zp", "x"))
    down_mine, down_theirs = exchange_down(w_down, later, core, zp, x, n_core, n_zp, n_x)

    mine = lax.dynamic_index_in_dim(picked, lax.axis_index("ez"), 0, keepdims=False)
    owner = mine // rows_dev
    places = jnp.arange(devices, dtype=jnp.int32)
    device_ids = places // split * split + places % n_zp * n_x + places // n_zp % n_x
    first = jnp.sum((owner[None, :] < device_ids[:, None]).astype(jnp.int32), axis=1)
    count = jnp.sum((owner[None, :] == device_ids[:, None]).astype(jnp.int32), axis=1)
    slot_ids = jnp.arange(most, dtype=jnp.int32)[None, :]
    target = jnp.where(slot_ids < count[:, None], first[:, None] + slot_ids, -1).reshape(-1)
    pack_mat = (jnp.arange(cap, dtype=jnp.int32)[:, None] == target[None, :]).astype(jnp.bfloat16)
    packed = jnp.dot(
        pack_mat, arrived[:, :, :piece].reshape(devices * most, piece), preferred_element_type=jnp.float32
    ).astype(jnp.bfloat16)

    rows = copy_to(packed, SHARE, split)
    gate = jnp.einsum("kpd,kdf->pf", rows, w_gate.reshape(split, piece, hidden_cols), preferred_element_type=jnp.float32)
    upper = jnp.einsum("kpd,kdf->pf", rows, w_up.reshape(split, piece, hidden_cols), preferred_element_type=jnp.float32)
    hidden = (jax.nn.silu(gate) * upper).astype(jnp.bfloat16)
    hidden, down_theirs, first_core = lax.optimization_barrier((hidden, down_theirs, core == 0))
    hidden = copy_to(hidden, SHARE, split)
    out_mine = jnp.einsum("kpf,kfd->pd", hidden, down_mine, preferred_element_type=jnp.float32).astype(jnp.bfloat16)
    out_theirs = jnp.einsum("kpf,kfd->pd", hidden, down_theirs, preferred_element_type=jnp.float32).astype(jnp.bfloat16)
    low = jnp.where(first_core, out_mine, out_theirs)
    high = jnp.where(first_core, out_theirs, out_mine)
    expert_out = jnp.concatenate([low, high], axis=1)
    spread = lax.dot_general(
        pack_mat, expert_out, (((0,), (0,)), ((), ())), preferred_element_type=jnp.float32
    ).astype(jnp.bfloat16)

    returned = lax.all_to_all(spread.reshape(devices, most, piece), TRADE, 0, 0, tiled=True)
    full_out = returned.reshape(experts, split, most, piece).transpose(0, 2, 1, 3).reshape(experts * most, width)

    loss = jnp.sum(arrived[:, :, piece:].astype(jnp.float32), axis=(0, 1))
    loss = add_partner(loss, "dp_0", 1)
    loss = lax.psum(loss, "dp_1")
    loss = add_partner(loss, "dp_0", 2)
    loss = add_partner(loss, "dp_0", 4)
    z_loss = jnp.sum(loss) / (n_dp * devices * rows_dev)

    window = logits[:, :experts].T
    peak = jnp.max(jnp.where(member, window, -1e30), axis=0, keepdims=True)
    peak = jnp.where(jnp.any(member, axis=0, keepdims=True), peak, 0.0)
    raised = jnp.where(member, jnp.exp(jnp.where(member, window - peak, -60.0)), 0.0)
    denom = jnp.sum(raised, axis=0, keepdims=True)
    combine = raised / jnp.where(denom > 0, denom, 1.0)
    weights = jnp.where(taken, combine[:, None, :], 0.0).reshape(experts * most, rows_dev)
    coarse = weights.astype(jnp.bfloat16)
    fine = (weights - coarse.astype(jnp.float32)).astype(jnp.bfloat16)
    mixed = lax.dot_general(
        jnp.concatenate([coarse, fine]),
        jnp.concatenate([full_out, full_out]),
        (((0,), (0,)), ((), ())),
        preferred_element_type=jnp.float32,
    )
    return (mixed.astype(jnp.bfloat16)[None], z_loss)


def solution(mesh):
    split = Mesh(mesh.devices.reshape(8, 2, 8, 2, 4), DP + EXPERT)
    in_specs = (
        P(DP, EXPERT, None),
        P(),
        P(DP, None, None),
        P(None, EXPERT),
        P(None, EXPERT),
        P(EXPERT, None),
    )
    out_specs = (P(DP, EXPERT, None), P())
    return jax.shard_map(layer, mesh=split, in_specs=in_specs, out_specs=out_specs, check_vma=False)
```
